32 devices in a mesh: data: 1 (over z), ffn: 4 (over y), hid: 8 (over x, core).
Axes of the slice: x: 4, y: 4, z: 1, core: 2. Of those that a mesh axis runs over, the one named last changes fastest.
The devices are a block of a 4x4x8 slice.
Arguments:
- x_in: bfloat16 [64, 4096], P('data', 'hid')
- gain_one: float32 [4096], P('hid')
- gain_two: float32 [4096], P('hid')
- w_gate: bfloat16 [4096, 11008], P('hid', 'ffn')
- w_up: bfloat16 [4096, 11008], P('hid', 'ffn')
- w_down: bfloat16 [11008, 4096], P('ffn', 'hid')
- w_qkv: bfloat16 [4096, 12288], P('hid', 'ffn')
- dx_out: bfloat16 [64, 4096], P('data', 'hid')
- d_qkv: bfloat16 [64, 12288], P('data', 'ffn')
Outputs:
- output 1: bfloat16 [64, 4096], P('data', 'hid')
- output 2: bfloat16 [4096, 11008], P(('data', 'hid'), 'ffn')
- output 3: bfloat16 [4096, 11008], P(('data', 'hid'), 'ffn')
- output 4: bfloat16 [11008, 4096], P(('data', 'ffn'), 'hid')
- output 5: bfloat16 [4096, 12288], P(('data', 'hid'), 'ffn')
- output 6: float32 [4096], P(('data', 'hid'))
- output 7: float32 [4096], P(('data', 'hid'))
All inputs are finite; a program needn't handle non-finite values.
Results may differ from the reference program's by a relative error of at most 0.00556686.
Values are sent between devices in bfloat16 or wider.
A program may use at most 768 MiB of HBM per device.

```python
import jax
import jax.numpy as jnp
from jax import lax

D_MODEL = 4096
D_FF = 11008
Q_HEADS = 32
KV_HEADS = 32
HEAD_DIM = 128
TOKENS = 64
QKV_WIDTH = (Q_HEADS + 2 * KV_HEADS) * HEAD_DIM
NORM_EPS = 1e-6


def norm_forward(z_val, gain_vec):
    inv_rms = lax.rsqrt(jnp.sum(z_val * z_val, axis=-1, keepdims=True) / D_MODEL + NORM_EPS)
    return inv_rms, (z_val * inv_rms * gain_vec).astype(jnp.bfloat16)


def norm_backward(z_val, gain_vec, inv_rms, d_norm):
    g_dn = gain_vec * d_norm
    dot_tok = jnp.sum(g_dn * z_val, axis=-1, keepdims=True)
    d_input = inv_rms * g_dn - z_val * (inv_rms ** 3) * (dot_tok / D_MODEL)
    d_gain = jnp.sum(d_norm * z_val * inv_rms, axis=0)
    return d_input, d_gain


def forward_states(x_in, gain_one, gain_two, w_gate, w_up, w_down):
    x_f32 = x_in.astype(jnp.float32)
    inv_one, normed_one = norm_forward(x_f32, gain_one)
    gate_pre = jnp.dot(normed_one, w_gate, preferred_element_type=jnp.float32)
    up_pre = jnp.dot(normed_one, w_up, preferred_element_type=jnp.float32)
    act_bf = (jax.nn.silu(gate_pre) * up_pre).astype(jnp.bfloat16)
    down_out = jnp.dot(act_bf, w_down, preferred_element_type=jnp.float32)
    resid_f32 = (x_f32 + down_out).astype(jnp.bfloat16).astype(jnp.float32)
    inv_two, normed_two = norm_forward(resid_f32, gain_two)
    return x_f32, inv_one, normed_one, gate_pre, up_pre, act_bf, resid_f32, inv_two, normed_two


def setup_inputs(seed: int = 0, part: int = 0) -> dict:
    shared_keys = jax.random.split(jax.random.key(seed), 6)
    part_keys = jax.random.split(jax.random.fold_in(jax.random.key(seed + 1), part), 6)
    positions = jnp.arange(D_MODEL, dtype=jnp.float32) / D_MODEL
    row_scale = jnp.exp(jax.random.uniform(part_keys[0], (TOKENS, 1), minval=-1.0, maxval=1.0))
    amplitude = jax.random.uniform(part_keys[1], (TOKENS, 1), minval=0.6, maxval=1.2)
    phase_off = jax.random.uniform(part_keys[2], (TOKENS, 1))
    profile = jnp.exp(amplitude * jnp.sin(2.0 * jnp.pi * (positions + phase_off)))
    x_in = (jax.random.normal(part_keys[3], (TOKENS, D_MODEL)) * row_scale * profile).astype(jnp.bfloat16)
    gain_one = jax.random.uniform(shared_keys[0], (D_MODEL,), minval=0.5, maxval=1.5)
    gain_two = jax.random.uniform(shared_keys[1], (D_MODEL,), minval=0.5, maxval=1.5)
    w_gate = (jax.random.normal(shared_keys[2], (D_MODEL, D_FF)) * D_MODEL ** -0.5).astype(jnp.bfloat16)
    w_up = (jax.random.normal(shared_keys[3], (D_MODEL, D_FF)) * D_MODEL ** -0.5).astype(jnp.bfloat16)
    w_down = (jax.random.normal(shared_keys[4], (D_FF, D_MODEL)) * D_FF ** -0.5).astype(jnp.bfloat16)
    w_qkv = (jax.random.normal(shared_keys[5], (D_MODEL, QKV_WIDTH)) * D_MODEL ** -0.5).astype(jnp.bfloat16)
    states = forward_states(x_in, gain_one, gain_two, w_gate, w_up, w_down)
    qkv_est = jnp.dot(states[8], w_qkv, preferred_element_type=jnp.float32)
    d_qkv = (qkv_est + 0.5 * jax.random.normal(part_keys[4], (TOKENS, QKV_WIDTH))).astype(jnp.bfloat16)
    dx_out = (3.0 * (states[6] - states[0]) + 0.5 * jax.random.normal(part_keys[5], (TOKENS, D_MODEL))).astype(jnp.bfloat16)
    return {"x_in": x_in, "gain_one": gain_one, "gain_two": gain_two, "w_gate": w_gate, "w_up": w_up, "w_down": w_down, "w_qkv": w_qkv, "dx_out": dx_out, "d_qkv": d_qkv}


def reference(x_in, gain_one, gain_two, w_gate, w_up, w_down, w_qkv, dx_out, d_qkv):
    x_f32, inv_one, normed_one, gate_pre, up_pre, act_bf, resid_f32, inv_two, normed_two = forward_states(x_in, gain_one, gain_two, w_gate, w_up, w_down)
    dw_qkv = jnp.dot(normed_two.T, d_qkv, preferred_element_type=jnp.float32).astype(jnp.bfloat16)
    d_normed_two = jnp.dot(d_qkv, w_qkv.T, preferred_element_type=jnp.float32)
    d_resid, d_gain_two = norm_backward(resid_f32, gain_two, inv_two, d_normed_two)
    d_res_tot = dx_out.astype(jnp.float32) + d_resid
    d_res_bf = d_res_tot.astype(jnp.bfloat16)
    dw_down = jnp.dot(act_bf.T, d_res_bf, preferred_element_type=jnp.float32).astype(jnp.bfloat16)
    d_act = jnp.dot(d_res_bf, w_down.T, preferred_element_type=jnp.float32)
    gate_sig = jax.nn.sigmoid(gate_pre)
    d_gate = (d_act * up_pre * gate_sig * (1.0 + gate_pre * (1.0 - gate_sig))).astype(jnp.bfloat16)
    d_up = (d_act * jax.nn.silu(gate_pre)).astype(jnp.bfloat16)
    dw_gate = jnp.dot(normed_one.T, d_gate, preferred_element_type=jnp.float32).astype(jnp.bfloat16)
    dw_up = jnp.dot(normed_one.T, d_up, preferred_element_type=jnp.float32).astype(jnp.bfloat16)
    d_normed_one = jnp.dot(d_gate, w_gate.T, preferred_element_type=jnp.float32) + jnp.dot(d_up, w_up.T, preferred_element_type=jnp.float32)
    d_in, d_gain_one = norm_backward(x_f32, gain_one, inv_one, d_normed_one)
    dx_in = (d_res_tot + d_in).astype(jnp.bfloat16)
    return (dx_in, dw_gate, dw_up, dw_down, dw_qkv, d_gain_one, d_gain_two)
```

```python
import functools

import jax
import jax.numpy as jnp
from jax import lax
from jax.experimental import pallas as pl
from jax.experimental.pallas import tpu as pltpu
from jax.sharding import PartitionSpec as P

NORM_EPS = 1e-6
F32 = jnp.float32
BF16 = jnp.bfloat16
MESH = pl.DeviceIdType.MESH
VMEM_LIMIT = 60 * 1024 * 1024
LANES = 128
CHUNK = 512


def dot_nn(a_mat, b_mat):
    return lax.dot_general(a_mat, b_mat, (((1,), (0,)), ((), ())), preferred_element_type=F32)


def dot_nt(a_mat, b_mat):
    return lax.dot_general(a_mat, b_mat, (((1,), (1,)), ((), ())), preferred_element_type=F32)


def dot_tn(a_mat, b_mat):
    return lax.dot_general(a_mat, b_mat, (((0,), (0,)), ((), ())), preferred_element_type=F32)


def half_width(width):
    return -(-width // (2 * LANES)) * LANES


def chunk_list(half):
    out, at = [], 0
    while at < half:
        size = min(CHUNK, half - at)
        out.append((at, size))
        at += size
    return out


def column_to_row(col, shift):
    tokens = col.shape[0]
    row_id = lax.broadcasted_iota(jnp.int32, (tokens, LANES), 0)
    lane_id = lax.broadcasted_iota(jnp.int32, (tokens, LANES), 1)
    return jnp.sum(jnp.where(lane_id == row_id + shift, jnp.broadcast_to(col, (tokens, LANES)), 0.0), axis=0, keepdims=True)


def row_to_column(row, tokens, shift):
    row_id = lax.broadcasted_iota(jnp.int32, (tokens, LANES), 0)
    lane_id = lax.broadcasted_iota(jnp.int32, (tokens, LANES), 1)
    return jnp.sum(jnp.where(lane_id == row_id + shift, jnp.broadcast_to(row, (tokens, LANES)), 0.0), axis=1, keepdims=True)


def chain_kernel(cfg, *refs):
    n_hid, n_ffn, tokens, width, ffw, qw = cfg["n_hid"], cfg["n_ffn"], cfg["tokens"], cfg["width"], cfg["ffw"], cfg["qw"]
    chips = n_hid // 2
    tb = tokens // chips
    half = half_width(ffw)
    chunks = chunk_list(half)
    nj = len(chunks)
    d_model = width * n_hid
    it = iter(refs)
    x_h, g1_h, g2_h, wg_h, wu_h, wd_h, wq_h, dxo_h, dq_h = [next(it) for _ in range(9)]
    dx_o, dg1_o, dg2_o, n1_o, n2_o, eb_o, a_o, dgu_o = [next(it) for _ in range(8)]
    x_v, g1_v, g2_v, wg_v, wu_v, wd_v, wq_v, dxo_v, dq_v = [next(it) for _ in range(9)]
    n1_v, n2_v, eb_v, e_v, dn2_v, stat1, stat2, stat3, dp_v, dn1_v, acc_v, dn2_s = [next(it) for _ in range(12)]
    part = [next(it) for _ in range(nj)]
    rx = [next(it) for _ in range(nj)]
    sb = [next(it) for _ in range(nj)]
    rr = [next(it) for _ in range(nj)]
    av = [next(it) for _ in range(nj)]
    sil = [next(it) for _ in range(nj)]
    pre = [next(it) for _ in range(nj)]
    part2 = [next(it) for _ in range(nj)]
    rx2 = [next(it) for _ in range(nj)]
    sb2 = [next(it) for _ in range(nj)]
    rr2 = [next(it) for _ in range(nj)]
    dgu = [next(it) for _ in range(nj)]
    load_sem, out_sem, send_sem, recv_sem, row_sem = [next(it) for _ in range(5)]

    hid = lax.axis_index("hid")
    ffn = lax.axis_index("ffn")
    chip = hid // 2
    core = hid % 2
    partner = chip * 2 + (1 - core)
    my_rows = pl.ds(pl.multiple_of(chip * tb, tb), tb)

    def hid_peer(d):
        return {"hid": (hid + d) % n_hid}

    def ffn_peer(d):
        return {"ffn": (ffn + d) % n_ffn}

    def chip_peer(d):
        return {"hid": ((chip + d) % chips) * 2 + core}

    n_sem = [0]
    sent = []

    def remote(src, dst, dev):
        s = n_sem[0]
        n_sem[0] += 1
        cp = pltpu.make_async_remote_copy(src_ref=src, dst_ref=dst, send_sem=send_sem.at[s], recv_sem=recv_sem.at[s], device_id=dev, device_id_type=MESH)
        cp.start()
        sent.append(cp)
        return cp

    loads = {}

    def load(name, src, dst):
        cp = pltpu.make_async_copy(src, dst, load_sem.at[len(loads)])
        cp.start()
        loads[name] = cp

    load("x", x_h, x_v)
    load("g1", g1_h, g1_v)
    load("dq", dq_h, dq_v)
    load("wq", wq_h, wq_v)
    load("wg", wg_h, wg_v)
    load("wu", wu_h, wu_v)
    load("wd", wd_h, wd_v.at[pl.ds(0, ffw)])
    load("g2", g2_h, g2_v)
    load("dxo", dxo_h, dxo_v)

    outs = []

    def store(src, dst):
        cp = pltpu.make_async_copy(src, dst, out_sem.at[len(outs)])
        cp.start()
        outs.append(cp)

    barrier = pltpu.get_barrier_semaphore()
    for d in range(1, n_hid):
        pl.semaphore_signal(barrier, inc=1, device_id=hid_peer(d), device_id_type=MESH)
    for d in range(1, n_ffn):
        pl.semaphore_signal(barrier, inc=1, device_id=ffn_peer(d), device_id_type=MESH)

    if 2 * half > ffw:
        wd_v[pl.ds(ffw, 2 * half - ffw), :] = jnp.zeros((2 * half - ffw, width), BF16)

    loads["x"].wait()
    x_f32 = x_v[...].astype(F32)
    stat1[pl.ds(hid, 1)] = column_to_row(jnp.sum(x_f32 * x_f32, axis=-1, keepdims=True), 0)[None]

    pl.semaphore_wait(barrier, n_hid - 1 + n_ffn - 1)
    st1 = [remote(stat1.at[hid], stat1.at[hid], hid_peer(d)) for d in range(1, n_hid)]
    for d in range(1, n_ffn):
        pl.semaphore_signal(row_sem, inc=1, device_id=ffn_peer(d), device_id_type=MESH)

    loads["dq"].wait()
    loads["wq"].wait()
    dn2_v[pl.ds(ffn, 1)] = dot_nt(dq_v[...], wq_v[...])[None]
    dn2_cp = [remote(dn2_v.at[ffn], dn2_v.at[ffn], ffn_peer(d)) for d in range(1, n_ffn)]

    loads["g1"].wait()
    for cp in st1:
        cp.wait_recv()
    ssq1 = row_to_column(jnp.sum(stat1[...], axis=0), tokens, 0)
    r1 = lax.rsqrt(ssq1 / d_model + NORM_EPS)
    n1_v[...] = (x_v[...].astype(F32) * r1 * g1_v[...]).astype(BF16)
    store(n1_v, n1_o)

    loads["wg"].wait()
    loads["wu"].wait()
    d2d = []
    for j, (c0, cw) in enumerate(chunks):
        for hf in range(2):
            lo = hf * half + c0
            valid = min(cw, ffw - lo)
            for gu, w_v in enumerate((wg_v, wu_v)):
                part[j][hf, gu, :, 0:valid] = dot_nn(n1_v[...], w_v[:, lo : lo + valid])
                if valid < cw:
                    part[j][hf, gu, :, valid:cw] = jnp.zeros((tokens, cw - valid), F32)
        d2d.append(remote(part[j].at[1 - core], rx[j], {"hid": partner}))
    rs = []
    for j, (c0, cw) in enumerate(chunks):
        d2d[j].wait_recv()
        for b in range(chips):
            rows = slice(b * tb, (b + 1) * tb)
            sb[j][b] = (part[j][core, :, rows, :] + rx[j][:, rows, :]).astype(sb[j].dtype)
        rs.append([remote(sb[j].at[(chip + d) % chips], rr[j].at[d - 1], chip_peer(d)) for d in range(1, chips)])
    ag = []
    for j, (c0, cw) in enumerate(chunks):
        for cp in rs[j]:
            cp.wait_recv()
        tot = part[j][core, :, my_rows, :] + rx[j][:, my_rows, :]
        for d in range(chips - 1):
            tot = tot + rr[j][d].astype(F32)
        gate, up = tot[0], tot[1]
        sig = jax.nn.sigmoid(gate)
        silu = gate * sig
        av[j][core, my_rows, :] = (silu * up).astype(BF16)
        ag.append([remote(av[j].at[core, my_rows], av[j].at[core, my_rows], chip_peer(d)) for d in range(1, chips)])
        sil[j][...] = silu
        pre[j][...] = up * sig * (1.0 + gate * (1.0 - sig))
    loads["wd"].wait()
    relay = []
    for j, (c0, cw) in enumerate(chunks):
        for cp in ag[j]:
            cp.wait_recv()
        relay.append(remote(av[j].at[core], av[j].at[core], {"hid": partner}))
        w_rows = pl.ds(pl.multiple_of(core * half, LANES) + c0, cw)
        prod = dot_nn(av[j][core], wd_v[w_rows, :])
        acc_v[...] = prod if j == 0 else acc_v[...] + prod
    for j, (c0, cw) in enumerate(chunks):
        relay[j].wait_recv()
        w_rows = pl.ds(pl.multiple_of((1 - core) * half, LANES) + c0, cw)
        acc_v[...] += dot_nn(av[j][1 - core], wd_v[w_rows, :])
    dp_v[pl.ds(ffn, 1)] = acc_v[...].astype(dp_v.dtype)[None]
    down_cp = [remote(dp_v.at[ffn], dp_v.at[ffn], ffn_peer(d)) for d in range(1, n_ffn)]
    for j, (c0, cw) in enumerate(chunks):
        store(av[j], a_o.at[:, :, pl.ds(c0, cw)])
    for cp in dn2_cp:
        cp.wait_recv()
    loads["g2"].wait()
    loads["dxo"].wait()
    dn2 = dn2_v[0]
    for i in range(1, n_ffn):
        dn2 = dn2 + dn2_v[i]
    dn2_s[...] = dn2
    for cp in down_cp:
        cp.wait_recv()
    down = dp_v[0].astype(F32)
    for i in range(1, n_ffn):
        down = down + dp_v[i].astype(F32)
    x2 = (x_v[...].astype(F32) + down).astype(BF16).astype(F32)
    gdn = g2_v[...] * dn2_s[...]
    stat2[pl.ds(hid, 1)] = (column_to_row(jnp.sum(x2 * x2, axis=-1, keepdims=True), 0) + column_to_row(jnp.sum(gdn * x2, axis=-1, keepdims=True), tokens))[None]
    st2 = [remote(stat2.at[hid], stat2.at[hid], hid_peer(d)) for d in range(1, n_hid)]
    acc_v[...] = x2
    for cp in st2:
        cp.wait_recv()
    tot2 = jnp.sum(stat2[...], axis=0)
    r2 = lax.rsqrt(row_to_column(tot2, tokens, 0) / d_model + NORM_EPS)
    c2 = row_to_column(tot2, tokens, tokens)
    x2 = acc_v[...]
    e_val = dxo_v[...].astype(F32) + (r2 * (g2_v[...] * dn2_s[...]) - x2 * (r2 * r2 * r2) * (c2 / d_model))
    e_v[...] = e_val
    eb_v[...] = e_val.astype(BF16)

    d2d = []
    for j, (c0, cw) in enumerate(chunks):
        for hf in range(2):
            part2[j][hf] = dot_nt(eb_v[...], wd_v[hf * half + c0 : hf * half + c0 + cw, :])
        d2d.append(remote(part2[j].at[1 - core], rx2[j], {"hid": partner}))
    rs = []
    for j, (c0, cw) in enumerate(chunks):
        d2d[j].wait_recv()
        for b in range(chips):
            rows = slice(b * tb, (b + 1) * tb)
            sb2[j][b] = (part2[j][core, rows, :] + rx2[j][rows, :]).astype(sb2[j].dtype)
        rs.append([remote(sb2[j].at[(chip + d) % chips], rr2[j].at[d - 1], chip_peer(d)) for d in range(1, chips)])
    store(eb_v, eb_o)
    x2 = acc_v[...]
    n2_v[...] = (x2 * r2 * g2_v[...]).astype(BF16)
    store(n2_v, n2_o)
    dg2_o[...] = jnp.sum(dn2_s[...] * x2 * r2, axis=0, keepdims=True)
    ag = []
    for j, (c0, cw) in enumerate(chunks):
        for cp in rs[j]:
            cp.wait_recv()
        d_act = part2[j][core, my_rows, :] + rx2[j][my_rows, :]
        for d in range(chips - 1):
            d_act = d_act + rr2[j][d].astype(F32)
        dgu[j][core, 0, my_rows, :] = (d_act * pre[j][...]).astype(BF16)
        dgu[j][core, 1, my_rows, :] = (d_act * sil[j][...]).astype(BF16)
        ag.append([remote(dgu[j].at[core, :, my_rows], dgu[j].at[core, :, my_rows], chip_peer(d)) for d in range(1, chips)])
    relay = []
    for j, (c0, cw) in enumerate(chunks):
        for cp in ag[j]:
            cp.wait_recv()
        relay.append(remote(dgu[j].at[core], dgu[j].at[core], {"hid": partner}))
    for j, (c0, cw) in enumerate(chunks):
        relay[j].wait_recv()
        prod = None
        for hf in range(2):
            lo = hf * half + c0
            valid = min(cw, ffw - lo)
            for gu, w_v in enumerate((wg_v, wu_v)):
                term = dot_nt(dgu[j][hf, gu, :, 0:valid], w_v[:, lo : lo + valid])
                prod = term if prod is None else prod + term
        acc_v[...] = prod if j == 0 else acc_v[...] + prod
    dn1p = acc_v[...]
    dn1_v[pl.ds(ffn, 1)] = dn1p.astype(dn1_v.dtype)[None]
    dn1_cp = [remote(dn1_v.at[ffn], dn1_v.at[ffn], ffn_peer(d)) for d in range(1, n_ffn)]
    me = ffn * n_hid + hid
    stat3[pl.ds(me, 1)] = column_to_row(jnp.sum(g1_v[...] * x_v[...].astype(F32) * dn1p, axis=-1, keepdims=True), 0)[None]
    pl.semaphore_wait(row_sem, n_ffn - 1)
    st3 = []
    for df in range(n_ffn):
        for d in range(n_hid):
            if df or d:
                st3.append(remote(stat3.at[me], stat3.at[me], {"ffn": (ffn + df) % n_ffn, "hid": (hid + d) % n_hid}))
    for j, (c0, cw) in enumerate(chunks):
        store(dgu[j], dgu_o.at[:, :, :, pl.ds(c0, cw)])
    for cp in dn1_cp:
        cp.wait_recv()
    dn1 = dn1_v[0].astype(F32)
    for i in range(1, n_ffn):
        dn1 = dn1 + dn1_v[i].astype(F32)
    x_f32 = x_v[...].astype(F32)
    dg1_o[...] = jnp.sum(dn1 * x_f32 * r1, axis=0, keepdims=True)
    for cp in st3:
        cp.wait_recv()
    c1 = row_to_column(jnp.sum(stat3[...], axis=0), tokens, 0)
    d_in = r1 * (g1_v[...] * dn1) - x_f32 * (r1 * r1 * r1) * (c1 / d_model)
    dx_o[...] = (e_v[...] + d_in).astype(BF16)
    for cp in sent:
        cp.wait_send()
    for cp in outs:
        cp.wait()


def weight_kernel(cfg, n1_r, n2_r, eb_r, a_r, dgu_r, dq_r, dwg_o, dwu_o, dwd_o, dwq_o, wg_s, wu_s, wd_s, wq_s, sem):
    tokens, width, ffw, qw = cfg["tokens"], cfg["width"], cfg["ffw"], cfg["qw"]
    half = half_width(ffw)
    rb = 128
    copies = []

    def flush(src, dst):
        cp = pltpu.make_async_copy(src, dst, sem.at[len(copies)])
        cp.start()
        copies.append(cp)

    for r0 in range(0, width, rb):
        rows = pl.ds(r0, rb)
        n2_t = n2_r[:, r0 : r0 + rb].T
        wq_s[rows, :] = dot_nn(n2_t, dq_r[...]).astype(BF16)
        flush(wq_s.at[rows], dwq_o.at[rows])
    for r0 in range(0, ffw, 2 * rb):
        size = min(2 * rb, ffw - r0)
        cuts = sorted({r0, min(max(half, r0), r0 + size), r0 + size})
        for lo, hi in zip(cuts[:-1], cuts[1:]):
            hf = lo // half
            wd_s[lo:hi, :] = dot_tn(a_r[hf, :, lo - hf * half : hi - hf * half], eb_r[...]).astype(BF16)
        rows = pl.ds(r0, size)
        flush(wd_s.at[rows], dwd_o.at[rows])
    for r0 in range(0, width, rb):
        rows = pl.ds(r0, rb)
        n1_t = n1_r[:, r0 : r0 + rb].T
        for gu, (s_r, o_r) in enumerate(((wg_s, dwg_o), (wu_s, dwu_o))):
            s_r[rows, 0:half] = dot_nn(n1_t, dgu_r[0, gu]).astype(BF16)
            s_r[rows, half:ffw] = dot_nn(n1_t, dgu_r[1, gu, :, 0 : ffw - half]).astype(BF16)
            flush(s_r.at[rows], o_r.at[rows])
    for cp in copies:
        cp.wait()


def solution(mesh):
    n_hid, n_ffn = mesh.shape["hid"], mesh.shape["ffn"]

    def local_step(x_in, gain_one, gain_two, w_gate, w_up, w_down, w_qkv, dx_out, d_qkv):
        tokens, width = x_in.shape
        ffw, qw = w_gate.shape[1], w_qkv.shape[1]
        half = half_width(ffw)
        chunks = chunk_list(half)
        chips = n_hid // 2
        tb = tokens // chips
        cfg = dict(n_hid=n_hid, n_ffn=n_ffn, tokens=tokens, width=width, ffw=ffw, qw=qw)
        vm = pltpu.VMEM
        per = lambda shape, dt: [vm(shape(cw), dt) for _, cw in chunks]
        scratch = [
            vm((tokens, width), BF16), vm((1, width), F32), vm((1, width), F32),
            vm((width, ffw), BF16), vm((width, ffw), BF16), vm((2 * half, width), BF16), vm((width, qw), BF16),
            vm((tokens, width), BF16), vm((tokens, qw), BF16),
            vm((tokens, width), BF16), vm((tokens, width), BF16), vm((tokens, width), BF16), vm((tokens, width), F32),
            vm((n_ffn, tokens, width), F32),
            vm((n_hid, 1, LANES), F32), vm((n_hid, 1, LANES), F32), vm((n_hid * n_ffn, 1, LANES), F32),
            vm((n_ffn, tokens, width), BF16), vm((n_ffn, tokens, width), BF16), vm((tokens, width), F32), vm((tokens, width), F32),
        ]
        scratch += per(lambda cw: (2, 2, tokens, cw), F32)
        scratch += per(lambda cw: (2, tokens, cw), F32)
        scratch += per(lambda cw: (chips, 2, tb, cw), BF16)
        scratch += per(lambda cw: (chips - 1, 2, tb, cw), BF16)
        scratch += per(lambda cw: (2, tokens, cw), BF16)
        scratch += per(lambda cw: (tb, cw), F32)
        scratch += per(lambda cw: (tb, cw), F32)
        scratch += per(lambda cw: (2, tokens, cw), F32)
        scratch += per(lambda cw: (tokens, cw), F32)
        scratch += per(lambda cw: (chips, tb, cw), BF16)
        scratch += per(lambda cw: (chips - 1, tb, cw), BF16)
        scratch += per(lambda cw: (2, 2, tokens, cw), BF16)
        n_copy = 2 * (n_hid - 1) + 3 * (n_ffn - 1) + len(chunks) * (4 + 4 * (chips - 1)) + n_hid * n_ffn - 1
        n_out = 3 + 2 * len(chunks)
        scratch += [pltpu.SemaphoreType.DMA((9,)), pltpu.SemaphoreType.DMA((n_out,)), pltpu.SemaphoreType.DMA((n_copy,)), pltpu.SemaphoreType.DMA((n_copy,)), pltpu.SemaphoreType.REGULAR]
        any_spec = pl.BlockSpec(memory_space=pl.ANY)
        vm_spec = pl.BlockSpec(memory_space=pltpu.VMEM)
        sds = jax.ShapeDtypeStruct
        dx_in, dg1, dg2, n1, n2, eb, a_full, dgu_full = pl.pallas_call(
            functools.partial(chain_kernel, cfg),
            out_shape=(
                sds((tokens, width), BF16), sds((1, width), F32), sds((1, width), F32),
                sds((tokens, width), BF16), sds((tokens, width), BF16), sds((tokens, width), BF16),
                sds((2, tokens, half), BF16), sds((2, 2, tokens, half), BF16),
            ),
            in_specs=[any_spec] * 9,
            out_specs=(vm_spec,) * 3 + (any_spec,) * 5,
            scratch_shapes=scratch,
            compiler_params=pltpu.CompilerParams(collective_id=0, has_side_effects=True, vmem_limit_bytes=VMEM_LIMIT),
            name="chain",
        )(x_in, gain_one.reshape(1, width), gain_two.reshape(1, width), w_gate, w_up, w_down, w_qkv, dx_out, d_qkv)
        n_flush = 3 * (width // 128) + -(-ffw // 256)
        dwg, dwu, dwd, dwq = pl.pallas_call(
            functools.partial(weight_kernel, cfg),
            out_shape=(sds((width, ffw), BF16), sds((width, ffw), BF16), sds((ffw, width), BF16), sds((width, qw), BF16)),
            in_specs=[vm_spec] * 6,
            out_specs=(any_spec,) * 4,
            scratch_shapes=[vm((width, ffw), BF16), vm((width, ffw), BF16), vm((ffw, width), BF16), vm((width, qw), BF16), pltpu.SemaphoreType.DMA((n_flush,))],
            compiler_params=pltpu.CompilerParams(vmem_limit_bytes=VMEM_LIMIT),
            name="weights",
        )(n1, n2, eb, a_full, dgu_full, d_qkv)
        return dx_in, dwg, dwu, dwd, dwq, dg1.reshape(width), dg2.reshape(width)

    tok_spec = P("data", "hid")
    in_specs = (tok_spec, P("hid"), P("hid"), P("hid", "ffn"), P("hid", "ffn"), P("ffn", "hid"), P("hid", "ffn"), tok_spec, P("data", "ffn"))
    out_specs = (tok_spec, P(("data", "hid"), "ffn"), P(("data", "hid"), "ffn"), P(("data", "ffn"), "hid"), P(("data", "hid"), "ffn"), P(("data", "hid")), P(("data", "hid")))
    return jax.shard_map(local_step, mesh=mesh, in_specs=in_specs, out_specs=out_specs, check_vma=False)
```

```python
import functools

import jax
import jax.numpy as jnp
from jax import lax
from jax.experimental import pallas as pl
from jax.experimental.pallas import tpu as pltpu
from jax.sharding import PartitionSpec as P

NORM_EPS = 1e-6
F32 = jnp.float32
BF16 = jnp.bfloat16
MESH = pl.DeviceIdType.MESH
VMEM_LIMIT = 60 * 1024 * 1024
LANES = 128
CHUNK = 384
ROW_BLOCK = 256
QKV_BLOCK = 128


def dot_nn(a_mat, b_mat):
    return lax.dot_general(a_mat, b_mat, (((1,), (0,)), ((), ())), preferred_element_type=F32)


def dot_nt(a_mat, b_mat):
    return lax.dot_general(a_mat, b_mat, (((1,), (1,)), ((), ())), preferred_element_type=F32)


def dot_tn(a_mat, b_mat):
    return lax.dot_general(a_mat, b_mat, (((0,), (0,)), ((), ())), preferred_element_type=F32)


def half_width(width):
    return -(-width // (2 * LANES)) * LANES


def chunk_list(half):
    tiles = half // LANES
    n = -(-tiles * LANES // CHUNK)
    sizes = [(tiles // n + (i >= n - tiles % n)) * LANES for i in range(n)]
    out, at = [], 0
    for size in sizes:
        out.append((at, size))
        at += size
    return out


def column_to_row(col, shift):
    tokens = col.shape[0]
    row_id = lax.broadcasted_iota(jnp.int32, (tokens, LANES), 0)
    lane_id = lax.broadcasted_iota(jnp.int32, (tokens, LANES), 1)
    return jnp.sum(jnp.where(lane_id == row_id + shift, jnp.broadcast_to(col, (tokens, LANES)), 0.0), axis=0, keepdims=True)


def row_to_column(row, tokens, shift):
    row_id = lax.broadcasted_iota(jnp.int32, (tokens, LANES), 0)
    lane_id = lax.broadcasted_iota(jnp.int32, (tokens, LANES), 1)
    return jnp.sum(jnp.where(lane_id == row_id + shift, jnp.broadcast_to(row, (tokens, LANES)), 0.0), axis=1, keepdims=True)


def chain_kernel(cfg, *refs):
    n_hid, n_ffn, tokens, width, ffw, qw = cfg["n_hid"], cfg["n_ffn"], cfg["tokens"], cfg["width"], cfg["ffw"], cfg["qw"]
    chips = n_hid // 2
    tb = tokens // chips
    half = half_width(ffw)
    chunks = chunk_list(half)
    nj = len(chunks)
    d_model = width * n_hid
    it = iter(refs)
    x_h, g1_h, g2_h, wg_h, wu_h, wd_h, wq_h, dxo_h, dq_h = [next(it) for _ in range(9)]
    dx_o, dg1_o, dg2_o, n1_o, n2_o, eb_o, a_o, dgu_o = [next(it) for _ in range(8)]
    x_v, g1_v, g2_v, wg_v, wu_v, wd_v, wq_v, dxo_v, dq_v = [next(it) for _ in range(9)]
    n1_v, n2_v, eb_v, e_v, dn2_v, stat1, stat2, stat3, dp_v, dn1_v, acc_v, dn2_s, acc2_v, x2_v = [next(it) for _ in range(14)]
    part = [next(it) for _ in range(nj)]
    rx = [next(it) for _ in range(nj)]
    sb = [next(it) for _ in range(nj)]
    rr = [next(it) for _ in range(nj)]
    av = [next(it) for _ in range(nj)]
    sil = [next(it) for _ in range(nj)]
    pre = [next(it) for _ in range(nj)]
    part2 = [next(it) for _ in range(nj)]
    rx2 = [next(it) for _ in range(nj)]
    sb2 = [next(it) for _ in range(nj)]
    rr2 = [next(it) for _ in range(nj)]
    dgu = [next(it) for _ in range(nj)]
    load_sem, out_sem, send_sem, recv_sem, row_sem = [next(it) for _ in range(5)]

    hid = lax.axis_index("hid")
    ffn = lax.axis_index("ffn")
    chip = hid // 2
    core = hid % 2
    partner = chip * 2 + (1 - core)
    my_rows = pl.ds(pl.multiple_of(chip * tb, tb), tb)

    def hid_peer(d):
        return {"hid": (hid + d) % n_hid}

    def ffn_peer(d):
        return {"ffn": (ffn + d) % n_ffn}

    def chip_peer(d):
        return {"hid": ((chip + d) % chips) * 2 + core}

    n_sem = [0]
    sent = []

    def remote(src, dst, dev):
        s = n_sem[0]
        n_sem[0] += 1
        cp = pltpu.make_async_remote_copy(src_ref=src, dst_ref=dst, send_sem=send_sem.at[s], recv_sem=recv_sem.at[s], device_id=dev, device_id_type=MESH)
        cp.start()
        sent.append(cp)
        return cp

    loads = {}

    def load(name, src, dst):
        cp = pltpu.make_async_copy(src, dst, load_sem.at[len(loads)])
        cp.start()
        loads[name] = cp

    load("x", x_h, x_v)
    load("g1", g1_h, g1_v)
    load("dq", dq_h, dq_v)
    load("wq", wq_h, wq_v)
    load("wg", wg_h, wg_v.at[pl.ds(0, ffw)])
    load("wu", wu_h, wu_v.at[pl.ds(0, ffw)])
    load("wd", wd_h, wd_v.at[pl.ds(0, ffw)])
    load("g2", g2_h, g2_v)
    load("dxo", dxo_h, dxo_v)

    outs = []

    def store(src, dst):
        cp = pltpu.make_async_copy(src, dst, out_sem.at[len(outs)])
        cp.start()
        outs.append(cp)

    barrier = pltpu.get_barrier_semaphore()
    for d in range(1, n_hid):
        pl.semaphore_signal(barrier, inc=1, device_id=hid_peer(d), device_id_type=MESH)
    for d in range(1, n_ffn):
        pl.semaphore_signal(barrier, inc=1, device_id=ffn_peer(d), device_id_type=MESH)

    if 2 * half > ffw:
        for w_v in (wg_v, wu_v, wd_v):
            w_v[pl.ds(ffw, 2 * half - ffw), :] = jnp.zeros((2 * half - ffw, width), BF16)

    loads["x"].wait()
    x_f32 = x_v[...].astype(F32)
    stat1[pl.ds(hid, 1)] = column_to_row(jnp.sum(x_f32 * x_f32, axis=-1, keepdims=True), 0)[None]

    pl.semaphore_wait(barrier, n_hid - 1 + n_ffn - 1)
    st1 = [remote(stat1.at[hid], stat1.at[hid], hid_peer(d)) for d in range(1, n_hid)]
    for d in range(1, n_ffn):
        pl.semaphore_signal(row_sem, inc=1, device_id=ffn_peer(d), device_id_type=MESH)

    loads["dq"].wait()
    loads["wq"].wait()
    dn2_v[pl.ds(ffn, 1)] = dot_nt(dq_v[...], wq_v[...])[None]
    dn2_cp = [remote(dn2_v.at[ffn], dn2_v.at[ffn], ffn_peer(d)) for d in range(1, n_ffn)]

    loads["g1"].wait()
    for cp in st1:
        cp.wait_recv()
    ssq1 = row_to_column(jnp.sum(stat1[...], axis=0), tokens, 0)
    r1 = lax.rsqrt(ssq1 / d_model + NORM_EPS)
    n1_v[...] = (x_v[...].astype(F32) * r1 * g1_v[...]).astype(BF16)
    store(n1_v, n1_o)

    loads["wg"].wait()
    loads["wu"].wait()
    d2d = []
    for j, (c0, cw) in enumerate(chunks):
        for hf in range(2):
            lo = hf * half + c0
            for gu, w_v in enumerate((wg_v, wu_v)):
                part[j][hf, gu] = dot_nt(n1_v[...], w_v[lo : lo + cw, :])
        d2d.append(remote(part[j].at[1 - core], rx[j], {"hid": partner}))
    rs = []
    for j, (c0, cw) in enumerate(chunks):
        d2d[j].wait_recv()
        for b in range(chips):
            rows = slice(b * tb, (b + 1) * tb)
            sb[j][b] = (part[j][core, :, rows, :] + rx[j][:, rows, :]).astype(sb[j].dtype)
        rs.append([remote(sb[j].at[(chip + d) % chips], rr[j].at[d - 1], chip_peer(d)) for d in range(1, chips)])
    ag = []
    for j, (c0, cw) in enumerate(chunks):
        for cp in rs[j]:
            cp.wait_recv()
        tot = part[j][core, :, my_rows, :] + rx[j][:, my_rows, :]
        for d in range(chips - 1):
            tot = tot + rr[j][d].astype(F32)
        gate, up = tot[0], tot[1]
        sig = jax.nn.sigmoid(gate)
        silu = gate * sig
        av[j][core, my_rows, :] = (silu * up).astype(BF16)
        ag.append([remote(av[j].at[core, my_rows], av[j].at[core, my_rows], chip_peer(d)) for d in range(1, chips)])
        sil[j][...] = silu
        pre[j][...] = up * sig * (1.0 + gate * (1.0 - sig))
    loads["wd"].wait()
    relay = []
    for j, (c0, cw) in enumerate(chunks):
        for cp in ag[j]:
            cp.wait_recv()
        relay.append(remote(av[j].at[core], av[j].at[core], {"hid": partner}))
        w_rows = pl.ds(pl.multiple_of(core * half, LANES) + c0, cw)
        prod = dot_nn(av[j][core], wd_v[w_rows, :])
        acc_v[...] = prod if j == 0 else acc_v[...] + prod
    for j, (c0, cw) in enumerate(chunks):
        relay[j].wait_recv()
        w_rows = pl.ds(pl.multiple_of((1 - core) * half, LANES) + c0, cw)
        acc_v[...] += dot_nn(av[j][1 - core], wd_v[w_rows, :])
    tf = tokens // n_ffn
    f_rows = pl.ds(pl.multiple_of(ffn * tf, tf), tf)
    down_cp = []
    for d in range(1, n_ffn):
        to = (ffn + d) % n_ffn
        down_cp.append(remote(acc_v.at[pl.ds(pl.multiple_of(to * tf, tf), tf)], dp_v.at[ffn], {"ffn": to}))
    dp_v[pl.ds(ffn, 1)] = acc_v[f_rows, :][None]
    for j, (c0, cw) in enumerate(chunks):
        store(av[j], a_o.at[:, :, pl.ds(c0, cw)])
    for cp in dn2_cp:
        cp.wait_recv()
    loads["g2"].wait()
    loads["dxo"].wait()
    dn2 = dn2_v[0]
    for i in range(1, n_ffn):
        dn2 = dn2 + dn2_v[i]
    dn2_s[...] = dn2
    pl.semaphore_wait(row_sem, n_ffn - 1)
    me = ffn * n_hid + hid

    def to_all(buf):
        cps = []
        for df in range(n_ffn):
            for d in range(n_hid):
                if df or d:
                    cps.append(remote(buf.at[me], buf.at[me], {"ffn": (ffn + df) % n_ffn, "hid": (hid + d) % n_hid}))
        return cps

    for cp in down_cp:
        cp.wait_recv()
    x2 = (x_v[f_rows, :].astype(F32) + jnp.sum(dp_v[...], axis=0)).astype(BF16)
    x2_v[f_rows, :] = x2
    x2_cp = [remote(x2_v.at[f_rows], x2_v.at[f_rows], ffn_peer(d)) for d in range(1, n_ffn)]
    x2 = x2.astype(F32)
    gdn = g2_v[...] * dn2_s[f_rows, :]
    stat2[pl.ds(me, 1)] = (column_to_row(jnp.sum(x2 * x2, axis=-1, keepdims=True), 0) + column_to_row(jnp.sum(gdn * x2, axis=-1, keepdims=True), tf))[None]
    st2 = to_all(stat2)
    for cp in x2_cp:
        cp.wait_recv()
    for cp in st2:
        cp.wait_recv()
    ssq2, c2 = [], []
    for i in range(n_ffn):
        tot2 = jnp.sum(stat2[i * n_hid : (i + 1) * n_hid], axis=0)
        ssq2.append(row_to_column(tot2, tf, 0))
        c2.append(row_to_column(tot2, tf, tf))
    ssq2, c2 = jnp.concatenate(ssq2, axis=0), jnp.concatenate(c2, axis=0)
    r2 = lax.rsqrt(ssq2 / d_model + NORM_EPS)
    x2 = x2_v[...].astype(F32)
    e_val = dxo_v[...].astype(F32) + (r2 * (g2_v[...] * dn2_s[...]) - x2 * (r2 * r2 * r2) * (c2 / d_model))
    e_v[...] = e_val
    eb_v[...] = e_val.astype(BF16)

    d2d = []
    for j, (c0, cw) in enumerate(chunks):
        for hf in range(2):
            part2[j][hf] = dot_nt(eb_v[...], wd_v[hf * half + c0 : hf * half + c0 + cw, :])
        d2d.append(remote(part2[j].at[1 - core], rx2[j], {"hid": partner}))
    rs = []
    for j, (c0, cw) in enumerate(chunks):
        d2d[j].wait_recv()
        for b in range(chips):
            rows = slice(b * tb, (b + 1) * tb)
            sb2[j][b] = (part2[j][core, rows, :] + rx2[j][rows, :]).astype(sb2[j].dtype)
        rs.append([remote(sb2[j].at[(chip + d) % chips], rr2[j].at[d - 1], chip_peer(d)) for d in range(1, chips)])
    store(eb_v, eb_o)
    x2 = x2_v[...].astype(F32)
    n2_v[...] = (x2 * r2 * g2_v[...]).astype(BF16)
    store(n2_v, n2_o)
    dg2_o[...] = jnp.sum(dn2_s[...] * x2 * r2, axis=0, keepdims=True)
    ag = []
    for j, (c0, cw) in enumerate(chunks):
        for cp in rs[j]:
            cp.wait_recv()
        d_act = part2[j][core, my_rows, :] + rx2[j][my_rows, :]
        for d in range(chips - 1):
            d_act = d_act + rr2[j][d].astype(F32)
        dgu[j][core, 0, my_rows, :] = (d_act * pre[j][...]).astype(BF16)
        dgu[j][core, 1, my_rows, :] = (d_act * sil[j][...]).astype(BF16)
        ag.append([remote(dgu[j].at[core, :, my_rows], dgu[j].at[core, :, my_rows], chip_peer(d)) for d in range(1, chips)])
    relay = []
    for j, (c0, cw) in enumerate(chunks):
        for cp in ag[j]:
            cp.wait_recv()
        relay.append(remote(dgu[j].at[core], dgu[j].at[core], {"hid": partner}))
    for j, (c0, cw) in enumerate(chunks):
        relay[j].wait_recv()
        prod = None
        for hf in range(2):
            lo = hf * half + c0
            for gu, w_v in enumerate((wg_v, wu_v)):
                term = dot_nn(dgu[j][hf, gu], w_v[lo : lo + cw, :])
                prod = term if prod is None else prod + term
        acc2_v[...] = prod if j == 0 else acc2_v[...] + prod
    dn1p = acc2_v[...]
    dn1_v[pl.ds(ffn, 1)] = dn1p.astype(dn1_v.dtype)[None]
    dn1_cp = [remote(dn1_v.at[ffn], dn1_v.at[ffn], ffn_peer(d)) for d in range(1, n_ffn)]
    stat3[pl.ds(me, 1)] = column_to_row(jnp.sum(g1_v[...] * x_v[...].astype(F32) * dn1p, axis=-1, keepdims=True), 0)[None]
    st3 = to_all(stat3)
    for j, (c0, cw) in enumerate(chunks):
        store(dgu[j], dgu_o.at[:, :, :, pl.ds(c0, cw)])
    for cp in dn1_cp:
        cp.wait_recv()
    dn1 = dn1_v[0].astype(F32)
    for i in range(1, n_ffn):
        dn1 = dn1 + dn1_v[i].astype(F32)
    x_f32 = x_v[...].astype(F32)
    dg1_o[...] = jnp.sum(dn1 * x_f32 * r1, axis=0, keepdims=True)
    for cp in st3:
        cp.wait_recv()
    c1 = row_to_column(jnp.sum(stat3[...], axis=0), tokens, 0)
    d_in = r1 * (g1_v[...] * dn1) - x_f32 * (r1 * r1 * r1) * (c1 / d_model)
    dx_o[...] = (e_v[...] + d_in).astype(BF16)
    for cp in sent:
        cp.wait_send()
    for cp in outs:
        cp.wait()


def weight_kernel(cfg, *refs):
    tokens, width, ffw, qw = cfg["tokens"], cfg["width"], cfg["ffw"], cfg["qw"]
    half = half_width(ffw)
    it = iter(refs)
    n1_h, n2_h, eb_h, a_h, dgu_h, dq_h, dx_r, dg1_r, dg2_r = [next(it) for _ in range(9)]
    dx_o, dg1_o, dg2_o, dwg_o, dwu_o, dwd_o, dwq_o = [next(it) for _ in range(7)]
    n1_r, n2_r, eb_r, a_r, dgu_r, dq_r, wg_s, wu_s, wd_s, wq_s, load_sem, sem = [next(it) for _ in range(12)]
    copies = []
    loads = []
    for i, (src, dst) in enumerate(((n2_h, n2_r), (dq_h, dq_r), (eb_h, eb_r), (a_h, a_r), (n1_h, n1_r), (dgu_h, dgu_r))):
        loads.append(pltpu.make_async_copy(src, dst, load_sem.at[i]))
        loads[-1].start()

    def flush(src, dst):
        cp = pltpu.make_async_copy(src, dst, sem.at[len(copies)])
        cp.start()
        copies.append(cp)

    def by_rows(lhs, rhs, out_s, out_o):
        for r0 in range(0, ffw, ROW_BLOCK):
            size = min(ROW_BLOCK, ffw - r0)
            cuts = sorted({r0, min(max(half, r0), r0 + size), r0 + size})
            for lo, hi in zip(cuts[:-1], cuts[1:]):
                hf = lo // half
                out_s[lo:hi, :] = dot_tn(lhs(hf, slice(lo - hf * half, hi - hf * half)), rhs[...]).astype(BF16)
            flush(out_s.at[pl.ds(r0, size)], out_o.at[pl.ds(r0, size)])

    dx_o[...] = dx_r[...]
    dg1_o[...] = dg1_r[...]
    dg2_o[...] = dg2_r[...]
    for cp in loads[0:2]:
        cp.wait()
    for r0 in range(0, width, QKV_BLOCK):
        wq_s[r0 : r0 + QKV_BLOCK, :] = dot_tn(n2_r[:, r0 : r0 + QKV_BLOCK], dq_r[...]).astype(BF16)
        flush(wq_s.at[pl.ds(r0, QKV_BLOCK)], dwq_o.at[pl.ds(r0, QKV_BLOCK)])
    for cp in loads[2:4]:
        cp.wait()
    by_rows(lambda hf, cols: a_r[hf, :, cols], eb_r, wd_s, dwd_o)
    for cp in loads[4:6]:
        cp.wait()
    by_rows(lambda hf, cols: dgu_r[hf, 0, :, cols], n1_r, wg_s, dwg_o)
    by_rows(lambda hf, cols: dgu_r[hf, 1, :, cols], n1_r, wu_s, dwu_o)
    for cp in copies:
        cp.wait()


def solution(mesh):
    n_hid, n_ffn = mesh.shape["hid"], mesh.shape["ffn"]

    def local_step(x_in, gain_one, gain_two, w_gate, w_up, w_down, w_qkv, dx_out, d_qkv):
        tokens, width = x_in.shape
        ffw, qw = w_gate.shape[1], w_qkv.shape[1]
        half = half_width(ffw)
        chunks = chunk_list(half)
        chips = n_hid // 2
        tb = tokens // chips
        cfg = dict(n_hid=n_hid, n_ffn=n_ffn, tokens=tokens, width=width, ffw=ffw, qw=qw)
        vm = pltpu.VMEM
        per = lambda shape, dt: [vm(shape(cw), dt) for _, cw in chunks]
        scratch = [
            vm((tokens, width), BF16), vm((1, width), F32), vm((1, width), F32),
            vm((2 * half, width), BF16), vm((2 * half, width), BF16), vm((2 * half, width), BF16), vm((width, qw), BF16),
            vm((tokens, width), BF16), vm((tokens, qw), BF16),
            vm((tokens, width), BF16), vm((tokens, width), BF16), vm((tokens, width), BF16), vm((tokens, width), F32),
            vm((n_ffn, tokens, width), F32),
            vm((n_hid, 1, LANES), F32), vm((n_hid * n_ffn, 1, LANES), F32), vm((n_hid * n_ffn, 1, LANES), F32),
            vm((n_ffn, tokens // n_ffn, width), F32), vm((n_ffn, tokens, width), BF16), vm((tokens, width), F32), vm((tokens, width), F32), vm((tokens, width), F32), vm((tokens, width), BF16),
        ]
        scratch += per(lambda cw: (2, 2, tokens, cw), F32)
        scratch += per(lambda cw: (2, tokens, cw), F32)
        scratch += per(lambda cw: (chips, 2, tb, cw), BF16)
        scratch += per(lambda cw: (chips - 1, 2, tb, cw), BF16)
        scratch += per(lambda cw: (2, tokens, cw), BF16)
        scratch += per(lambda cw: (tb, cw), F32)
        scratch += per(lambda cw: (tb, cw), F32)
        scratch += per(lambda cw: (2, tokens, cw), F32)
        scratch += per(lambda cw: (tokens, cw), F32)
        scratch += per(lambda cw: (chips, tb, cw), BF16)
        scratch += per(lambda cw: (chips - 1, tb, cw), BF16)
        scratch += per(lambda cw: (2, 2, tokens, cw), BF16)
        n_copy = n_hid - 1 + 4 * (n_ffn - 1) + len(chunks) * (4 + 4 * (chips - 1)) + 2 * (n_hid * n_ffn - 1)
        n_out = 3 + 2 * len(chunks)
        scratch += [pltpu.SemaphoreType.DMA((9,)), pltpu.SemaphoreType.DMA((n_out,)), pltpu.SemaphoreType.DMA((n_copy,)), pltpu.SemaphoreType.DMA((n_copy,)), pltpu.SemaphoreType.REGULAR]
        any_spec = pl.BlockSpec(memory_space=pl.ANY)
        vm_spec = pl.BlockSpec(memory_space=pltpu.VMEM)
        sds = jax.ShapeDtypeStruct
        dx_in, dg1, dg2, n1, n2, eb, a_full, dgu_full = pl.pallas_call(
            functools.partial(chain_kernel, cfg),
            out_shape=(
                sds((tokens, width), BF16), sds((1, width), F32), sds((1, width), F32),
                sds((tokens, width), BF16), sds((tokens, width), BF16), sds((tokens, width), BF16),
                sds((2, tokens, half), BF16), sds((2, 2, tokens, half), BF16),
            ),
            in_specs=[any_spec] * 9,
            out_specs=(vm_spec,) * 3 + (any_spec,) * 5,
            scratch_shapes=scratch,
            compiler_params=pltpu.CompilerParams(collective_id=0, has_side_effects=True, vmem_limit_bytes=VMEM_LIMIT),
            name="chain",
        )(x_in, gain_one.reshape(1, width), gain_two.reshape(1, width), w_gate.T, w_up.T, w_down, w_qkv, dx_out, d_qkv)
        n_flush = width // QKV_BLOCK + 3 * -(-ffw // ROW_BLOCK)
        dx_in, dg1, dg2, dwg, dwu, dwd, dwq = pl.pallas_call(
            functools.partial(weight_kernel, cfg),
            out_shape=(
                sds((tokens, width), BF16), sds((1, width), F32), sds((1, width), F32),
                sds((ffw, width), BF16), sds((ffw, width), BF16), sds((ffw, width), BF16), sds((width, qw), BF16),
            ),
            in_specs=[any_spec] * 6 + [vm_spec] * 3,
            out_specs=(vm_spec,) * 3 + (any_spec,) * 4,
            scratch_shapes=[
                vm((tokens, width), BF16), vm((tokens, width), BF16), vm((tokens, width), BF16),
                vm((2, tokens, half), BF16), vm((2, 2, tokens, half), BF16), vm((tokens, qw), BF16),
                vm((ffw, width), BF16), vm((ffw, width), BF16), vm((ffw, width), BF16), vm((width, qw), BF16),
                pltpu.SemaphoreType.DMA((6,)), pltpu.SemaphoreType.DMA((n_flush,)),
            ],
            compiler_params=pltpu.CompilerParams(vmem_limit_bytes=VMEM_LIMIT),
            name="weights",
        )(n1, n2, eb, a_full, dgu_full, d_qkv, dx_in, dg1, dg2)
        return dx_in, dwg.T, dwu.T, dwd, dwq, dg1.reshape(width), dg2.reshape(width)

    tok_spec = P("data", "hid")
    in_specs = (tok_spec, P("hid"), P("hid"), P("hid", "ffn"), P("hid", "ffn"), P("ffn", "hid"), P("hid", "ffn"), tok_spec, P("data", "ffn"))
    out_specs = (tok_spec, P(("data", "hid"), "ffn"), P(("data", "hid"), "ffn"), P(("data", "ffn"), "hid"), P(("data", "hid"), "ffn"), P(("data", "hid")), P(("data", "hid")))
    return jax.shard_map(local_step, mesh=mesh, in_specs=in_specs, out_specs=out_specs, check_vma=False)
```

```python
import functools

import jax
import jax.numpy as jnp
from jax import lax
from jax.experimental import pallas as pl
from jax.experimental.pallas import tpu as pltpu
from jax.sharding import PartitionSpec as P

NORM_EPS = 1e-6
F32 = jnp.float32
BF16 = jnp.bfloat16
MESH = pl.DeviceIdType.MESH
VMEM_LIMIT = 55_300_000
FLUSH_LIMIT = 2 * 1024 * 1024
FLUSH_PARTS = 4
LANES = 128
CHUNK = 384
QKV_BLOCK = 128


def dot_nn(a_mat, b_mat):
    return lax.dot_general(a_mat, b_mat, (((1,), (0,)), ((), ())), preferred_element_type=F32)


def dot_nt(a_mat, b_mat):
    return lax.dot_general(a_mat, b_mat, (((1,), (1,)), ((), ())), preferred_element_type=F32)


def dot_tn(a_mat, b_mat):
    return lax.dot_general(a_mat, b_mat, (((0,), (0,)), ((), ())), preferred_element_type=F32)


def half_width(width):
    return -(-width // (2 * LANES)) * LANES


def chunk_list(half):
    tiles = half // LANES
    n = -(-tiles * LANES // CHUNK)
    sizes = [(tiles // n + (i >= n - tiles % n)) * LANES for i in range(n)]
    out, at = [], 0
    for size in sizes:
        out.append((at, size))
        at += size
    return out


def far_first(n):
    return sorted(range(1, n), key=lambda d: -min(d, n - d))


def column_to_row(col, shift):
    tokens = col.shape[0]
    row_id = lax.broadcasted_iota(jnp.int32, (tokens, LANES), 0)
    lane_id = lax.broadcasted_iota(jnp.int32, (tokens, LANES), 1)
    return jnp.sum(jnp.where(lane_id == row_id + shift, jnp.broadcast_to(col, (tokens, LANES)), 0.0), axis=0, keepdims=True)


def row_to_column(row, tokens, shift):
    row_id = lax.broadcasted_iota(jnp.int32, (tokens, LANES), 0)
    lane_id = lax.broadcasted_iota(jnp.int32, (tokens, LANES), 1)
    return jnp.sum(jnp.where(lane_id == row_id + shift, jnp.broadcast_to(row, (tokens, LANES)), 0.0), axis=1, keepdims=True)


def chain_kernel(cfg, *refs):
    n_hid, n_ffn, tokens, width, ffw, qw = cfg["n_hid"], cfg["n_ffn"], cfg["tokens"], cfg["width"], cfg["ffw"], cfg["qw"]
    chips = n_hid // 2
    tb = tokens // chips
    half = half_width(ffw)
    chunks = chunk_list(half)
    nj = len(chunks)
    d_model = width * n_hid
    it = iter(refs)
    x_h, g1_h, g2_h, wg_h, wu_h, wd_h, wq_h, dxo_h, dq_h = [next(it) for _ in range(9)]
    dx_o, dg1_o, dg2_o, dwg_o, dwu_o, dwd_o, dwq_o = [next(it) for _ in range(7)]
    x_v, g1_v, g2_v, wg_v, wu_v, wd_v, wq_v, dxo_v, dq_v = [next(it) for _ in range(9)]
    n1_v, n2_v, eb_v, e_v, dn2_v, stat1, stat2, stat3, dp_v, dn1_v, acc_v, dn2_s, acc2_v, x2_v = [next(it) for _ in range(14)]
    part = [next(it) for _ in range(nj)]
    rx = [next(it) for _ in range(nj)]
    sb = [next(it) for _ in range(nj)]
    rr = [next(it) for _ in range(nj)]
    av = [next(it) for _ in range(nj)]
    sil = [next(it) for _ in range(nj)]
    pre = [next(it) for _ in range(nj)]
    part2 = [next(it) for _ in range(nj)]
    rx2 = [next(it) for _ in range(nj)]
    sb2 = [next(it) for _ in range(nj)]
    rr2 = [next(it) for _ in range(nj)]
    dgu = [next(it) for _ in range(nj)]
    load_sem, send_sem, recv_sem, row_sem = [next(it) for _ in range(4)]

    hid = lax.axis_index("hid")
    ffn = lax.axis_index("ffn")
    chip = hid // 2
    core = hid % 2
    partner = chip * 2 + (1 - core)
    my_rows = pl.ds(pl.multiple_of(chip * tb, tb), tb)

    def hid_peer(d):
        return {"hid": (hid + d) % n_hid}

    def ffn_peer(d):
        return {"ffn": (ffn + d) % n_ffn}

    def chip_peer(d):
        return {"hid": ((chip + d) % chips) * 2 + core}

    n_sem = [0]
    sent = []

    def remote(src, dst, dev):
        s = n_sem[0]
        n_sem[0] += 1
        cp = pltpu.make_async_remote_copy(src_ref=src, dst_ref=dst, send_sem=send_sem.at[s], recv_sem=recv_sem.at[s], device_id=dev, device_id_type=MESH)
        cp.start()
        sent.append(cp)
        return cp

    loads = {}

    def load(name, src, dst):
        cp = pltpu.make_async_copy(src, dst, load_sem.at[len(loads)])
        cp.start()
        loads[name] = cp

    load("x", x_h, x_v)
    load("g1", g1_h, g1_v)
    load("dq", dq_h, dq_v)
    load("wq", wq_h, wq_v)
    load("wg", wg_h, wg_v.at[pl.ds(0, ffw)])
    load("wu", wu_h, wu_v.at[pl.ds(0, ffw)])
    load("wd", wd_h, wd_v.at[pl.ds(0, ffw)])
    load("g2", g2_h, g2_v)
    load("dxo", dxo_h, dxo_v)

    def by_rows(lhs, rhs, out):
        for hf in range(2):
            for j, (c0, cw) in enumerate(chunks):
                lo = hf * half + c0
                size = min(cw, ffw - lo)
                out[lo : lo + size, :] = dot_tn(lhs(j, hf)[:, 0:size], rhs[...]).astype(BF16)

    barrier = pltpu.get_barrier_semaphore()
    for d in range(1, n_hid):
        pl.semaphore_signal(barrier, inc=1, device_id=hid_peer(d), device_id_type=MESH)
    for d in range(1, n_ffn):
        pl.semaphore_signal(barrier, inc=1, device_id=ffn_peer(d), device_id_type=MESH)

    if 2 * half > ffw:
        for w_v in (wg_v, wu_v, wd_v):
            w_v[pl.ds(ffw, 2 * half - ffw), :] = jnp.zeros((2 * half - ffw, width), BF16)

    loads["x"].wait()
    x_f32 = x_v[...].astype(F32)
    stat1[pl.ds(hid, 1)] = column_to_row(jnp.sum(x_f32 * x_f32, axis=-1, keepdims=True), 0)[None]

    pl.semaphore_wait(barrier, n_hid - 1 + n_ffn - 1)
    st1 = [remote(stat1.at[hid], stat1.at[hid], hid_peer(d)) for d in far_first(n_hid)]
    for d in range(1, n_ffn):
        pl.semaphore_signal(row_sem, inc=1, device_id=ffn_peer(d), device_id_type=MESH)

    loads["dq"].wait()
    loads["wq"].wait()
    dn2_v[pl.ds(ffn, 1)] = dot_nt(dq_v[...], wq_v[...])[None]
    dn2_cp = [remote(dn2_v.at[ffn], dn2_v.at[ffn], ffn_peer(d)) for d in far_first(n_ffn)]

    loads["g1"].wait()
    for cp in st1:
        cp.wait_recv()
    ssq1 = row_to_column(jnp.sum(stat1[...], axis=0), tokens, 0)
    r1 = lax.rsqrt(ssq1 / d_model + NORM_EPS)
    n1_v[...] = (x_v[...].astype(F32) * r1 * g1_v[...]).astype(BF16)

    loads["wg"].wait()
    loads["wu"].wait()
    d2d = []
    for j, (c0, cw) in enumerate(chunks):
        for hf in range(2):
            lo = hf * half + c0
            for gu, w_v in enumerate((wg_v, wu_v)):
                part[j][hf, gu] = dot_nt(n1_v[...], w_v[lo : lo + cw, :])
        d2d.append(remote(part[j].at[1 - core], rx[j], {"hid": partner}))
    rs = []
    for j, (c0, cw) in enumerate(chunks):
        d2d[j].wait_recv()
        for b in range(chips):
            rows = slice(b * tb, (b + 1) * tb)
            sb[j][b] = (part[j][core, :, rows, :] + rx[j][:, rows, :]).astype(sb[j].dtype)
        rs.append([remote(sb[j].at[(chip + d) % chips], rr[j].at[d - 1], chip_peer(d)) for d in far_first(chips)])
    ag = []
    for j, (c0, cw) in enumerate(chunks):
        for cp in rs[j]:
            cp.wait_recv()
        tot = part[j][core, :, my_rows, :] + rx[j][:, my_rows, :]
        for d in range(chips - 1):
            tot = tot + rr[j][d].astype(F32)
        gate, up = tot[0], tot[1]
        sig = jax.nn.sigmoid(gate)
        silu = gate * sig
        av[j][core, my_rows, :] = (silu * up).astype(BF16)
        ag.append([remote(av[j].at[core, my_rows], av[j].at[core, my_rows], chip_peer(d)) for d in far_first(chips)])
        sil[j][...] = silu
        pre[j][...] = up * sig * (1.0 + gate * (1.0 - sig))
    loads["wd"].wait()
    relay = []
    for j, (c0, cw) in enumerate(chunks):
        for cp in ag[j]:
            cp.wait_recv()
        relay.append(remote(av[j].at[core], av[j].at[core], {"hid": partner}))
        w_rows = pl.ds(pl.multiple_of(core * half, LANES) + c0, cw)
        prod = dot_nn(av[j][core], wd_v[w_rows, :])
        acc_v[...] = prod if j == 0 else acc_v[...] + prod
    for j, (c0, cw) in enumerate(chunks):
        relay[j].wait_recv()
        w_rows = pl.ds(pl.multiple_of((1 - core) * half, LANES) + c0, cw)
        acc_v[...] += dot_nn(av[j][1 - core], wd_v[w_rows, :])
    tf = tokens // n_ffn
    f_rows = pl.ds(pl.multiple_of(ffn * tf, tf), tf)
    down_cp = []
    for d in range(1, n_ffn):
        to = (ffn + d) % n_ffn
        down_cp.append(remote(acc_v.at[pl.ds(pl.multiple_of(to * tf, tf), tf)], dp_v.at[ffn], {"ffn": to}))
    dp_v[pl.ds(ffn, 1)] = acc_v[f_rows, :][None]
    for cp in dn2_cp:
        cp.wait_recv()
    loads["g2"].wait()
    loads["dxo"].wait()
    dn2 = dn2_v[0]
    for i in range(1, n_ffn):
        dn2 = dn2 + dn2_v[i]
    dn2_s[...] = dn2
    pl.semaphore_wait(row_sem, n_ffn - 1)
    me = ffn * n_hid + hid

    def to_all(buf):
        far = lambda d, n: min(d, n - d)
        hops = sorted(((df, dc) for df in range(n_ffn) for dc in range(chips)), key=lambda p: -far(p[0], n_ffn) - far(p[1], chips))
        cps = []
        for df, dc in hops:
            for flip in range(2):
                if df or dc or flip:
                    to_hid = (chip + dc) % chips * 2 + (1 - core if flip else core)
                    cps.append(remote(buf.at[me], buf.at[me], {"ffn": (ffn + df) % n_ffn, "hid": to_hid}))
        return cps

    for cp in down_cp:
        cp.wait_recv()
    x2 = (x_v[f_rows, :].astype(F32) + jnp.sum(dp_v[...], axis=0)).astype(BF16)
    x2_v[f_rows, :] = x2
    x2_cp = [remote(x2_v.at[f_rows], x2_v.at[f_rows], ffn_peer(d)) for d in far_first(n_ffn)]
    x2 = x2.astype(F32)
    gdn = g2_v[...] * dn2_s[f_rows, :]
    stat2[pl.ds(me, 1)] = (column_to_row(jnp.sum(x2 * x2, axis=-1, keepdims=True), 0) + column_to_row(jnp.sum(gdn * x2, axis=-1, keepdims=True), tf))[None]
    st2 = to_all(stat2)
    for cp in x2_cp:
        cp.wait_recv()
    for cp in st2:
        cp.wait_recv()
    ssq2, c2 = [], []
    for i in range(n_ffn):
        tot2 = jnp.sum(stat2[i * n_hid : (i + 1) * n_hid], axis=0)
        ssq2.append(row_to_column(tot2, tf, 0))
        c2.append(row_to_column(tot2, tf, tf))
    ssq2, c2 = jnp.concatenate(ssq2, axis=0), jnp.concatenate(c2, axis=0)
    r2 = lax.rsqrt(ssq2 / d_model + NORM_EPS)
    x2 = x2_v[...].astype(F32)
    e_val = dxo_v[...].astype(F32) + (r2 * (g2_v[...] * dn2_s[...]) - x2 * (r2 * r2 * r2) * (c2 / d_model))
    e_v[...] = e_val
    eb_v[...] = e_val.astype(BF16)

    d2d = []
    for j, (c0, cw) in enumerate(chunks):
        for hf in range(2):
            part2[j][hf] = dot_nt(eb_v[...], wd_v[hf * half + c0 : hf * half + c0 + cw, :])
        d2d.append(remote(part2[j].at[1 - core], rx2[j], {"hid": partner}))
    rs = []
    for j, (c0, cw) in enumerate(chunks):
        d2d[j].wait_recv()
        for b in range(chips):
            rows = slice(b * tb, (b + 1) * tb)
            sb2[j][b] = (part2[j][core, rows, :] + rx2[j][rows, :]).astype(sb2[j].dtype)
        rs.append([remote(sb2[j].at[(chip + d) % chips], rr2[j].at[d - 1], chip_peer(d)) for d in far_first(chips)])
    x2 = x2_v[...].astype(F32)
    n2_v[...] = (x2 * r2 * g2_v[...]).astype(BF16)
    for r0 in range(0, width, QKV_BLOCK):
        dwq_o[r0 : r0 + QKV_BLOCK, :] = dot_tn(n2_v[:, r0 : r0 + QKV_BLOCK], dq_v[...]).astype(BF16)
    dg2_o[...] = jnp.sum(dn2_s[...] * x2 * r2, axis=0, keepdims=True)
    ag = []
    for j, (c0, cw) in enumerate(chunks):
        for cp in rs[j]:
            cp.wait_recv()
        d_act = part2[j][core, my_rows, :] + rx2[j][my_rows, :]
        for d in range(chips - 1):
            d_act = d_act + rr2[j][d].astype(F32)
        dgu[j][core, 0, my_rows, :] = (d_act * pre[j][...]).astype(BF16)
        dgu[j][core, 1, my_rows, :] = (d_act * sil[j][...]).astype(BF16)
        ag.append([remote(dgu[j].at[core, :, my_rows], dgu[j].at[core, :, my_rows], chip_peer(d)) for d in far_first(chips)])
    by_rows(lambda j, hf: av[j][hf], eb_v, dwd_o)
    relay = []
    for j, (c0, cw) in enumerate(chunks):
        for cp in ag[j]:
            cp.wait_recv()
        relay.append(remote(dgu[j].at[core], dgu[j].at[core], {"hid": partner}))
    for j, (c0, cw) in enumerate(chunks):
        relay[j].wait_recv()
        prod = None
        for hf in range(2):
            lo = hf * half + c0
            for gu, w_v in enumerate((wg_v, wu_v)):
                term = dot_nn(dgu[j][hf, gu], w_v[lo : lo + cw, :])
                prod = term if prod is None else prod + term
        acc2_v[...] = prod if j == 0 else acc2_v[...] + prod
    dn1p = acc2_v[...]
    dn1_v[pl.ds(ffn, 1)] = dn1p.astype(dn1_v.dtype)[None]
    dn1_cp = [remote(dn1_v.at[ffn], dn1_v.at[ffn], ffn_peer(d)) for d in far_first(n_ffn)]
    stat3[pl.ds(me, 1)] = column_to_row(jnp.sum(g1_v[...] * x_v[...].astype(F32) * dn1p, axis=-1, keepdims=True), 0)[None]
    st3 = to_all(stat3)
    by_rows(lambda j, hf: dgu[j][hf, 0], n1_v, dwg_o)
    by_rows(lambda j, hf: dgu[j][hf, 1], n1_v, dwu_o)
    for cp in dn1_cp:
        cp.wait_recv()
    dn1 = dn1_v[0].astype(F32)
    for i in range(1, n_ffn):
        dn1 = dn1 + dn1_v[i].astype(F32)
    x_f32 = x_v[...].astype(F32)
    dg1_o[...] = jnp.sum(dn1 * x_f32 * r1, axis=0, keepdims=True)
    for cp in st3:
        cp.wait_recv()
    c1 = row_to_column(jnp.sum(stat3[...], axis=0), tokens, 0)
    d_in = r1 * (g1_v[...] * dn1) - x_f32 * (r1 * r1 * r1) * (c1 / d_model)
    dx_o[...] = (e_v[...] + d_in).astype(BF16)
    for cp in sent:
        cp.wait_send()


def flush_pieces(shape):
    rows = shape[0] // FLUSH_PARTS if shape[0] % (16 * FLUSH_PARTS) == 0 else shape[0]
    return [pl.ds(r0, rows) for r0 in range(0, shape[0], rows)]


def flush_kernel(*refs):
    n_out = len(refs) // 2
    sem = refs[-1]
    copies = []
    for src, dst in zip(refs[:n_out], refs[n_out : 2 * n_out]):
        for rows in flush_pieces(src.shape):
            copies.append(pltpu.make_async_copy(src.at[rows], dst.at[rows], sem.at[len(copies)]))
            copies[-1].start()
    for cp in copies:
        cp.wait()


def solution(mesh):
    n_hid, n_ffn = mesh.shape["hid"], mesh.shape["ffn"]

    def local_step(x_in, gain_one, gain_two, w_gate, w_up, w_down, w_qkv, dx_out, d_qkv):
        tokens, width = x_in.shape
        ffw, qw = w_gate.shape[1], w_qkv.shape[1]
        half = half_width(ffw)
        chunks = chunk_list(half)
        chips = n_hid // 2
        tb = tokens // chips
        cfg = dict(n_hid=n_hid, n_ffn=n_ffn, tokens=tokens, width=width, ffw=ffw, qw=qw)
        vm = pltpu.VMEM
        per = lambda shape, dt: [vm(shape(cw), dt) for _, cw in chunks]
        scratch = [
            vm((tokens, width), BF16), vm((1, width), F32), vm((1, width), F32),
            vm((2 * half, width), BF16), vm((2 * half, width), BF16), vm((2 * half, width), BF16), vm((width, qw), BF16),
            vm((tokens, width), BF16), vm((tokens, qw), BF16),
            vm((tokens, width), BF16), vm((tokens, width), BF16), vm((tokens, width), BF16), vm((tokens, width), F32),
            vm((n_ffn, tokens, width), F32),
            vm((n_hid, 1, LANES), F32), vm((n_hid * n_ffn, 1, LANES), F32), vm((n_hid * n_ffn, 1, LANES), F32),
            vm((n_ffn, tokens // n_ffn, width), F32), vm((n_ffn, tokens, width), BF16), vm((tokens, width), F32), vm((tokens, width), F32), vm((tokens, width), F32), vm((tokens, width), BF16),
        ]
        scratch += per(lambda cw: (2, 2, tokens, cw), F32)
        scratch += per(lambda cw: (2, tokens, cw), F32)
        scratch += per(lambda cw: (chips, 2, tb, cw), BF16)
        scratch += per(lambda cw: (chips - 1, 2, tb, cw), BF16)
        scratch += per(lambda cw: (2, tokens, cw), BF16)
        scratch += per(lambda cw: (tb, cw), F32)
        scratch += per(lambda cw: (tb, cw), F32)
        scratch += per(lambda cw: (2, tokens, cw), F32)
        scratch += per(lambda cw: (tokens, cw), F32)
        scratch += per(lambda cw: (chips, tb, cw), BF16)
        scratch += per(lambda cw: (chips - 1, tb, cw), BF16)
        scratch += per(lambda cw: (2, 2, tokens, cw), BF16)
        n_copy = n_hid - 1 + 4 * (n_ffn - 1) + len(chunks) * (4 + 4 * (chips - 1)) + 2 * (n_hid * n_ffn - 1)
        scratch += [pltpu.SemaphoreType.DMA((9,)), pltpu.SemaphoreType.DMA((n_copy,)), pltpu.SemaphoreType.DMA((n_copy,)), pltpu.SemaphoreType.REGULAR]
        any_spec = pl.BlockSpec(memory_space=pltpu.HBM)
        vm_spec = pl.BlockSpec(memory_space=pltpu.VMEM)
        sds = jax.ShapeDtypeStruct
        results = (
            ((tokens, width), BF16), ((1, width), F32), ((1, width), F32),
            ((ffw, width), BF16), ((ffw, width), BF16), ((ffw, width), BF16), ((width, qw), BF16),
        )
        outs = pl.pallas_call(
            functools.partial(chain_kernel, cfg),
            out_shape=tuple(vm(shape, dt) for shape, dt in results),
            in_specs=[any_spec] * 9,
            out_specs=(vm_spec,) * 7,
            scratch_shapes=scratch,
            compiler_params=pltpu.CompilerParams(collective_id=0, has_side_effects=True, vmem_limit_bytes=VMEM_LIMIT),
            name="chain",
        )(x_in, gain_one.reshape(1, width), gain_two.reshape(1, width), w_gate.T, w_up.T, w_down, w_qkv, dx_out, d_qkv)
        dx_in, dg1, dg2, dwg, dwu, dwd, dwq = pl.pallas_call(
            flush_kernel,
            out_shape=tuple(sds(shape, dt) for shape, dt in results),
            in_specs=[vm_spec] * 7,
            out_specs=(any_spec,) * 7,
            scratch_shapes=[pltpu.SemaphoreType.DMA((sum(len(flush_pieces(shape)) for shape, _ in results),))],
            compiler_params=pltpu.CompilerParams(vmem_limit_bytes=FLUSH_LIMIT),
            name="flush",
        )(*outs)
        return dx_in, dwg.T, dwu.T, dwd, dwq, dg1.reshape(width), dg2.reshape(width)

    tok_spec = P("data", "hid")
    in_specs = (tok_spec, P("hid"), P("hid"), P("hid", "ffn"), P("hid", "ffn"), P("ffn", "hid"), P("hid", "ffn"), tok_spec, P("data", "ffn"))
    out_specs = (tok_spec, P(("data", "hid"), "ffn"), P(("data", "hid"), "ffn"), P(("data", "ffn"), "hid"), P(("data", "hid"), "ffn"), P(("data", "hid")), P(("data", "hid")))
    return jax.shard_map(local_step, mesh=mesh, in_specs=in_specs, out_specs=out_specs, check_vma=False)
```
